32 devices in a mesh: seq: 8 (over z, x), head: 4 (over y, core).
Axes of the slice: x: 2, y: 2, z: 4, core: 2. Of those that a mesh axis runs over, the one named last changes fastest.
Arguments:
- query_rows: bfloat16 [16384, 1024], P('seq', 'head'), may hold values from -8 to 8
- key_rows: bfloat16 [16384, 1024], P('seq', 'head'), may hold values from -6 to 6
- value_rows: bfloat16 [16384, 1024], P('seq', 'head'), may hold values from -12 to 12
- out_grad: bfloat16 [16384, 1024], P('seq', 'head'), may hold values from -12 to 12
- block_perm: int32 [8, 64], P('head'), may hold values from 0 to 63, as said below
- cut_count: int32 [8], P('head'), may hold values from 1 to 4, as said below
- norm_gain: float32 [1024], P('head'), may hold values from 0.1 to 1.9
Outputs:
- normed_out: bfloat16 [16384, 1024], P('seq', 'head')
- query_grad: bfloat16 [16384, 1024], P('seq', 'head')
- key_grad: bfloat16 [16384, 1024], P('seq', 'head')
- value_grad: bfloat16 [16384, 1024], P('seq', 'head')
- gain_grad: float32 [1024], P('head')
The draws below stay inside these ranges and needn't reach their ends.
Inputs may be any that keep to these rules, and one draw needn't show every extreme that they name: `block_perm`: each row is a permutation of 0 to 63. For every head, of the 8 blocks d * 8 to (d + 1) * 8 - 1, at most 1 are paired with blocks of one range s * 8 to (s + 1) * 8 - 1, and some pair (d, s) reaches 1. `cut_count`: some head has exactly 4.
All inputs are finite; a program needn't handle non-finite values.
Results may differ from the reference program's by a relative error of at most 0.0071.
Values may be sent and summed in bfloat16 or wider, within the bound.
A program may use at most 128 MiB of HBM per device.

```python
import math
import jax
import jax.numpy as jnp
from jax import lax

DH = 128
H = 8
BLOCK = 256
KCUT = 4
BLK_DEV = 8
SEQ = 16384
N_SEQ = 8


def draw_block_perm(key, part):

    def one_head(head_key):
        parts = jax.random.split(head_key, 4)
        alpha = jax.random.permutation(parts[0], N_SEQ)
        beta = jax.random.permutation(parts[1], N_SEQ)
        sigma = jax.random.permutation(parts[2], N_SEQ)
        local_index = jnp.arange(BLK_DEV)
        offset = sigma[local_index % N_SEQ]
        target = jnp.arange(N_SEQ)
        source = alpha[(beta[target][:, None] + offset[None, :]) % N_SEQ]
        shuffles = jax.vmap(lambda row_key: jax.random.permutation(row_key, BLK_DEV))(jax.random.split(parts[3], N_SEQ))
        chosen = shuffles[source, local_index[None, :]]
        return (source * BLK_DEV + chosen).reshape(N_SEQ * BLK_DEV)
    head_keys = jax.random.split(jax.random.fold_in(key, 11), H)
    return jax.vmap(one_head)(head_keys).astype(jnp.int32)


def draw_cut_count(key, part):
    counts = jax.random.randint(jax.random.fold_in(key, 21), (H,), 1, KCUT + 1)
    full_head = jax.random.randint(jax.random.fold_in(key, 22), (), 0, H)
    return jnp.where(jnp.arange(H) == full_head, KCUT, counts).astype(jnp.int32)


def draw_query_rows(key, part):
    row_scale = jnp.exp(jax.random.uniform(jax.random.fold_in(key, 2), (SEQ, 1), minval=math.log(0.3), maxval=math.log(3.0)))
    base = jax.random.normal(jax.random.fold_in(key, 1), (SEQ, H * DH)) * row_scale
    return jnp.clip(base, -8.0, 8.0).astype(jnp.bfloat16)


def draw_key_rows(key, part):
    base = jax.random.normal(jax.random.fold_in(key, 3), (SEQ, H * DH))
    return jnp.clip(base, -6.0, 6.0).astype(jnp.bfloat16)


def draw_value_rows(key, part):
    head_of = (jnp.arange(H * DH) // DH).astype(jnp.float32)
    base = jax.random.normal(jax.random.fold_in(key, 4), (SEQ, H * DH))
    jitter = jnp.exp(jax.random.uniform(jax.random.fold_in(key, 5), (H,), minval=math.log(0.8), maxval=math.log(1.25)))
    head_scale = 3.0 ** (head_of / (H - 1)) * jitter[jnp.arange(H * DH) // DH]
    return jnp.clip(base * head_scale[None, :], -12.0, 12.0).astype(jnp.bfloat16)


def draw_out_grad(key, part):
    place = jnp.arange(SEQ).astype(jnp.float32) / SEQ
    base = jax.random.normal(jax.random.fold_in(key, 6), (SEQ, H * DH))
    token_scale = jnp.exp(jax.random.uniform(jax.random.fold_in(key, 7), (SEQ,), minval=math.log(0.5), maxval=math.log(2.0)))
    base = base * (3.0 ** place * token_scale)[:, None]
    return jnp.clip(base, -12.0, 12.0).astype(jnp.bfloat16)


def setup_inputs(seed: int = 0) -> dict:
    arg_keys = jax.random.split(jax.random.key(seed), 8)
    return {
        "query_rows": draw_query_rows(jax.random.fold_in(arg_keys[7], 71), 0),
        "key_rows": draw_key_rows(jax.random.fold_in(arg_keys[7], 71), 0),
        "value_rows": draw_value_rows(jax.random.fold_in(arg_keys[7], 71), 0),
        "out_grad": draw_out_grad(jax.random.fold_in(arg_keys[7], 71), 0),
        "block_perm": draw_block_perm(jax.random.fold_in(arg_keys[7], 71), 0),
        "cut_count": draw_cut_count(jax.random.fold_in(arg_keys[7], 71), 0),
        "norm_gain": jnp.clip(1.0 + 0.18 * jax.random.normal(arg_keys[6], (H * DH,), jnp.float32), 0.1, 1.9),
    }


def split_heads(rows):
    tokens = rows.shape[0]
    return rows.reshape(tokens // BLOCK, BLOCK, H, DH).transpose(2, 0, 1, 3)

def merge_heads(parts):
    return parts.transpose(1, 2, 0, 3).reshape(parts.shape[1] * parts.shape[2], parts.shape[0] * parts.shape[3])

def attend(query, own_rows, paired_rows, cutoff_rows, live):
    width = query.shape[-1]
    span = own_rows.shape[1]
    count = cutoff_rows.shape[0]
    query_f = query.astype(jnp.float32)
    own = jnp.einsum('gqd,gkd->gqk', query_f, own_rows[..., :width].astype(jnp.float32))
    pair = jnp.einsum('gqd,gkd->gqk', query_f, paired_rows[..., :width].astype(jnp.float32))
    cut = jnp.einsum('gqd,ckd->gqck', query_f, cutoff_rows[..., :width].astype(jnp.float32))
    cut = cut.reshape(query.shape[0], query.shape[1], count * span)
    scores = jnp.concatenate([own, pair, cut], axis=-1) * DH ** (-0.5)
    open_keys = jnp.concatenate([jnp.ones((2 * span,), jnp.bool_), jnp.repeat(live, span)])
    scores = jnp.where(open_keys, scores, -1e+30)
    top = lax.optimization_barrier(jnp.max(scores, axis=-1))
    weights = jnp.exp(scores - top[..., None])
    total = lax.optimization_barrier(jnp.sum(weights, axis=-1))
    return (weights / total[..., None], top, total)

def mix_values(weights, own_rows, paired_rows, cutoff_rows):
    width = own_rows.shape[-1] // 2
    span = own_rows.shape[1]
    count = cutoff_rows.shape[0]
    weights_f = weights.astype(jnp.float32)
    result = jnp.einsum('gqk,gkd->gqd', weights_f[..., :span], own_rows[..., width:].astype(jnp.float32))
    result = result + jnp.einsum('gqk,gkd->gqd', weights_f[..., span:2 * span], paired_rows[..., width:].astype(jnp.float32))
    cut = weights_f[..., 2 * span:].reshape(weights.shape[0], weights.shape[1], count, span)
    return result + jnp.einsum('gqck,ckd->gqd', cut, cutoff_rows[..., width:].astype(jnp.float32))

def head_forward(items):
    query, own_blocks, perm, count = items
    paired = own_blocks[perm]
    cutoff = own_blocks[perm[:KCUT]]
    live = jnp.arange(KCUT) < count
    groups = query.shape[0] // 2

    def step(pieces):
        query_part, own_part, pair_part = pieces
        prob, top, total = attend(query_part, own_part, pair_part, cutoff, live)
        weights = prob.astype(jnp.bfloat16)
        return mix_values(weights, own_part, pair_part, cutoff).astype(jnp.bfloat16)
    result = lax.map(step, (query.reshape(groups, 2, BLOCK, DH), own_blocks.reshape(groups, 2, BLOCK, 2 * DH), paired.reshape(groups, 2, BLOCK, 2 * DH)))
    return result.reshape(query.shape)

def head_backward(items):
    query, own_blocks, perm, count, cotangent = items
    paired = own_blocks[perm]
    cutoff = own_blocks[perm[:KCUT]]
    live = jnp.arange(KCUT) < count
    groups = query.shape[0] // 2
    span = BLOCK

    def step(carry, pieces):
        query_part, own_part, pair_part, cot_part = pieces
        prob, top, total = attend(query_part, own_part, pair_part, cutoff, live)
        weights = prob.astype(jnp.bfloat16).astype(jnp.float32)
        cot_f = cot_part.astype(jnp.float32)
        query_f = query_part.astype(jnp.float32)
        dprob = jnp.concatenate([jnp.einsum('gqd,gkd->gqk', cot_f, own_part[..., DH:].astype(jnp.float32)), jnp.einsum('gqd,gkd->gqk', cot_f, pair_part[..., DH:].astype(jnp.float32)), jnp.einsum('gqd,ckd->gqck', cot_f, cutoff[..., DH:].astype(jnp.float32)).reshape(2, span, KCUT * span)], axis=-1)
        delta = lax.optimization_barrier(jnp.sum(prob * dprob, axis=-1))
        dscore = (prob * (dprob - delta[..., None]) * DH ** (-0.5)).astype(jnp.bfloat16).astype(jnp.float32)
        cut_score = dscore[..., 2 * span:].reshape(2, span, KCUT, span)
        cut_weight = weights[..., 2 * span:].reshape(2, span, KCUT, span)
        query_grad = jnp.einsum('gqk,gkd->gqd', dscore[..., :span], own_part[..., :DH].astype(jnp.float32))
        query_grad = query_grad + jnp.einsum('gqk,gkd->gqd', dscore[..., span:2 * span], pair_part[..., :DH].astype(jnp.float32))
        query_grad = query_grad + jnp.einsum('gqck,ckd->gqd', cut_score, cutoff[..., :DH].astype(jnp.float32))
        own_grad = jnp.concatenate([jnp.einsum('gqk,gqd->gkd', dscore[..., :span], query_f), jnp.einsum('gqk,gqd->gkd', weights[..., :span], cot_f)], axis=-1)
        pair_grad = jnp.concatenate([jnp.einsum('gqk,gqd->gkd', dscore[..., span:2 * span], query_f), jnp.einsum('gqk,gqd->gkd', weights[..., span:2 * span], cot_f)], axis=-1)
        cut_grad = jnp.concatenate([jnp.einsum('gqck,gqd->ckd', cut_score, query_f), jnp.einsum('gqck,gqd->ckd', cut_weight, cot_f)], axis=-1)
        return (carry + cut_grad, (query_grad.astype(jnp.bfloat16), own_grad, pair_grad))
    start = jnp.zeros((KCUT, span, 2 * DH), jnp.float32)
    cut_sum, outputs = lax.scan(step, start, (query.reshape(groups, 2, BLOCK, DH), own_blocks.reshape(groups, 2, BLOCK, 2 * DH), paired.reshape(groups, 2, BLOCK, 2 * DH), cotangent.reshape(groups, 2, BLOCK, DH)))
    query_grad, own_grad, pair_grad = outputs
    own_grad = own_grad.reshape(own_blocks.shape)
    pair_grad = pair_grad.reshape(own_blocks.shape)
    pair_round = lax.optimization_barrier(pair_grad.astype(jnp.bfloat16)).astype(jnp.float32)
    pair_term = jnp.zeros(own_blocks.shape, jnp.float32).at[perm].set(pair_round)
    cut_term = jnp.zeros(own_blocks.shape, jnp.float32).at[perm[:KCUT]].add(cut_sum)
    total_grad = (own_grad + pair_term + cut_term).astype(jnp.bfloat16)
    return (query_grad.reshape(query.shape), total_grad)

def reference(query_rows, key_rows, value_rows, out_grad, block_perm, cut_count, norm_gain):
    query_h = split_heads(query_rows)
    own_blocks = jnp.concatenate([split_heads(key_rows), split_heads(value_rows)], axis=-1)
    attn = lax.map(head_forward, (query_h, own_blocks, block_perm, cut_count))
    attn_f = attn.astype(jnp.float32)
    grad_f = split_heads(out_grad).astype(jnp.float32)
    gain = norm_gain.reshape(H, 1, 1, DH)
    features = H * DH
    square_sum = lax.optimization_barrier(jnp.sum(attn_f * attn_f, axis=(0, 3)))
    mix_sum = lax.optimization_barrier(jnp.sum(gain * grad_f * attn_f, axis=(0, 3)))
    scale_row = lax.rsqrt(square_sum / features + 1e-06)[None, :, :, None]
    normed = (attn_f * scale_row * gain).astype(jnp.bfloat16)
    gain_grad = lax.optimization_barrier(jnp.sum(grad_f * attn_f * scale_row, axis=(1, 2))).reshape(H * DH)
    cotangent = (scale_row * gain * grad_f - attn_f * scale_row ** 3 * mix_sum[None, :, :, None] / features).astype(jnp.bfloat16)
    query_grad, total_grad = lax.map(head_backward, (query_h, own_blocks, block_perm, cut_count, cotangent))
    return (merge_heads(normed), merge_heads(query_grad), merge_heads(total_grad[..., :DH]), merge_heads(total_grad[..., DH:]), gain_grad)
```

```python
import math

import jax
import jax.numpy as jnp
from jax import lax
from jax.experimental import pallas as pl
from jax.experimental.pallas import tpu as pltpu
from jax.sharding import PartitionSpec as P

BLOCK = 256
KCUT = 4
F32 = jnp.float32
BF16 = jnp.bfloat16
NT = (((1,), (1,)), ((), ()))
TN = (((0,), (0,)), ((), ()))
NN = (((1,), (0,)), ((), ()))
VMEM_LIMIT = 60 * 1024 * 1024
MESH = pl.DeviceIdType.MESH


def dot(a, b, dims):
    return lax.dot_general(a, b, dims, preferred_element_type=F32)


class Dims:
    def __init__(self, heads, width, blocks, slots, head_devs):
        self.heads = heads
        self.width = width
        self.blocks = blocks
        self.slots = slots
        self.head_devs = head_devs
        self.inner = 2
        self.outer = slots // 2
        self.stat_rows = 8 * (-(-2 * heads // 8))


def scratch_of(d):
    H, W, NB, S, L = d.heads, d.width, d.blocks, d.slots, d.outer
    dma = pltpu.SemaphoreType.DMA
    return dict(
        q=pltpu.VMEM((NB, BLOCK, H * W), BF16),
        k=pltpu.VMEM((NB, BLOCK, H * W), BF16),
        v=pltpu.VMEM((NB, BLOCK, H * W), BF16),
        g=pltpu.VMEM((NB, BLOCK, H * W), BF16),
        kv_send=pltpu.VMEM((S, H, BLOCK, 2 * W), BF16),
        kv_recv=pltpu.VMEM((S, H, BLOCK, 2 * W), BF16),
        cut=pltpu.VMEM((S, H, BLOCK, 2 * W), BF16),
        q_send=pltpu.VMEM((S, H, BLOCK, W), BF16),
        q_recv=pltpu.VMEM((S, H, BLOCK, W), BF16),
        cot_send=pltpu.VMEM((S, H, BLOCK, W), BF16),
        cot_recv=pltpu.VMEM((S, H, BLOCK, W), BF16),
        cst_send=pltpu.VMEM((S, d.stat_rows, BLOCK), F32),
        cst_recv=pltpu.VMEM((S, d.stat_rows, BLOCK), F32),
        ck=pltpu.VMEM((H, KCUT * BLOCK, W), BF16),
        cv=pltpu.VMEM((H, KCUT * BLOCK, W), BF16),
        s_buf=pltpu.VMEM((H, 1 + KCUT, BLOCK, BLOCK), F32),
        acc=pltpu.VMEM((H, NB, W, BLOCK), F32),
        soft=pltpu.VMEM((H, NB, 8, BLOCK), F32),
        attn_t=pltpu.VMEM((H, NB, W, BLOCK), BF16),
        g_t=pltpu.VMEM((H, NB, W, BLOCK), BF16),
        gain_t=pltpu.VMEM((H, W, BLOCK), F32),
        gain_acc=pltpu.VMEM((H, W, BLOCK), F32),
        sum_mine=pltpu.VMEM((2 * NB, BLOCK), F32),
        sum_recv=pltpu.VMEM((d.head_devs, 2 * NB, BLOCK), F32),
        row=pltpu.VMEM((2 * NB, BLOCK), F32),
        stat=pltpu.VMEM((NB, d.stat_rows, BLOCK), F32),
        cot=pltpu.VMEM((H, NB, BLOCK, W), BF16),
        cut_sum=pltpu.VMEM((H, KCUT, BLOCK, 2 * W), F32),
        x_send=pltpu.VMEM((H, L, BLOCK, 2 * W), BF16),
        x_recv=pltpu.VMEM((H, L, BLOCK, 2 * W), BF16),
        z_send=pltpu.VMEM((H, L, BLOCK, 2 * W), BF16),
        z_recv=pltpu.VMEM((H, L, BLOCK, 2 * W), BF16),
        dkv=pltpu.VMEM((NB, H, BLOCK, 2 * W), F32),
        gain_mine=pltpu.VMEM((8, H * W), F32),
        gain_recv=pltpu.VMEM((S, 8, H * W), F32),
        norm_buf=pltpu.VMEM((NB, BLOCK, H * W), BF16),
        dq_buf=pltpu.VMEM((NB, BLOCK, H * W), BF16),
        dk_buf=pltpu.VMEM((NB, BLOCK, H * W), BF16),
        dv_buf=pltpu.VMEM((NB, BLOCK, H * W), BF16),
        in_sem=dma((4,)),
        out_sem=dma((4,)),
        own_sem=dma((4,)),
        kv_ss=dma((S,)),
        kv_rs=dma((S,)),
        q_ss=dma((S,)),
        q_rs=dma((S,)),
        cot_ss=dma((S,)),
        cot_rs=dma((S,)),
        cst_ss=dma((S,)),
        cst_rs=dma((S,)),
        up_ss=dma((L,)),
        down_ss=dma((L,)),
        across_ss=dma((L,)),
        cut_rs=dma((S,)),
        sum_ss=dma((d.head_devs,)),
        sum_rs=dma((d.head_devs,)),
        x_ss=dma((H,)),
        x_rs=dma((H,)),
        z_ss=dma((H, L)),
        z_rs=dma((H, L)),
        gain_ss=dma((S,)),
        gain_rs=dma((S,)),
    )


def make_kernel(d, names):
    H, W, NB, S, L, HD = d.heads, d.width, d.blocks, d.slots, d.outer, d.head_devs
    features = HD * H * W
    scale = W ** (-0.5)
    factor = scale * math.log2(math.e)

    def cols(h):
        return slice(h * W, (h + 1) * W)

    def kernel(perm, count, q_hbm, k_hbm, v_hbm, g_hbm, gain, norm_hbm, dq_hbm, dk_hbm, dv_hbm, gain_out, *scratch):
        m = dict(zip(names, scratch))
        pos = lax.axis_index("seq")
        hpos = lax.axis_index("head")
        o = lax.div(pos, 2)
        i = lax.rem(pos, 2)

        def local(src, dst, sem):
            return pltpu.make_async_copy(src, dst, sem)

        def remote(src, dst, ss, rs, seq=None, head=None):
            target = {"seq": seq} if seq is not None else {"head": head}
            return pltpu.make_async_remote_copy(
                src_ref=src, dst_ref=dst, send_sem=ss, recv_sem=rs, device_id=target, device_id_type=MESH
            )

        loads = [
            local(src, m[name], m["in_sem"].at[n])
            for n, (src, name) in enumerate([(k_hbm, "k"), (v_hbm, "v"), (q_hbm, "q"), (g_hbm, "g")])
        ]
        for copy in loads:
            copy.start()

        barrier = pltpu.get_barrier_semaphore()
        for n in range(1, S):
            pl.semaphore_signal(barrier, inc=1, device_id={"seq": lax.rem(pos + n, S)}, device_id_type=MESH)
        for n in range(1, HD):
            pl.semaphore_signal(barrier, inc=1, device_id={"head": lax.rem(hpos + n, HD)}, device_id_type=MESH)

        kv_idx = []
        q_idx = []
        slot_of = []
        for h in range(H):
            kv_row = []
            q_row = []
            slot_row = []
            for s in range(S):
                idx = jnp.int32(0)
                qi = jnp.int32(0)
                valid = jnp.int32(-1)
                for b in range(NB):
                    p = perm[h, s * NB + b]
                    mine = lax.div(p, NB) == pos
                    idx = jnp.where(mine, lax.rem(p, NB), idx)
                    valid = jnp.where(mine, lax.rem(p, NB), valid)
                    there = lax.div(perm[h, pos * NB + b], NB) == s
                    qi = jnp.where(there, b, qi)
                slot_row.append(valid)
                kv_row.append(idx)
                q_row.append(qi)
            kv_idx.append(kv_row)
            q_idx.append(q_row)
            slot_of.append(slot_row)
        cut_dev = [[lax.div(perm[h, c], NB) for c in range(KCUT)] for h in range(H)]
        cut_local = []
        cut_has = []
        closed = []
        for h in range(H):
            where = jnp.int32(0)
            has = jnp.int32(0)
            for c in range(KCUT):
                mine = cut_dev[h][c] == pos
                where = jnp.where(mine, lax.rem(perm[h, c], NB), where)
                has = jnp.where(mine, 1, has)
            cut_local.append(where)
            cut_has.append(has)
            closed.append([jnp.where(count[h] > c, jnp.float32(0), jnp.float32(1e30)) for c in range(KCUT)])

        loads[0].wait()
        loads[1].wait()
        k, v, q, g = m["k"], m["v"], m["q"], m["g"]
        for h in range(H):
            r = cut_local[h]
            m["cut"][pos, h, :, :W] = k[r, :, cols(h)]
            m["cut"][pos, h, :, W:] = v[r, :, cols(h)]
        for h in range(H):
            for s in range(S):
                r = kv_idx[h][s]
                m["kv_send"][s, h, :, :W] = k[r, :, cols(h)]
                m["kv_send"][s, h, :, W:] = v[r, :, cols(h)]
        pl.semaphore_wait(barrier, S - 1 + HD - 1)

        def cut_copy(outer, sem, target):
            slot = outer * 2 + i
            return remote(m["cut"].at[slot], m["cut"].at[slot], sem, m["cut_rs"].at[slot], seq=target)

        def cut_arrive(slot):
            remote(m["cut"].at[slot], m["cut"].at[slot], m["across_ss"].at[0], m["cut_rs"].at[slot], seq=pos).wait_recv()

        def kv_copy(n):
            peer = lax.rem(pos + n, S)
            return remote(m["kv_send"].at[peer], m["kv_recv"].at[pos], m["kv_ss"].at[n], m["kv_rs"].at[n], seq=peer)

        def q_copy(n):
            peer = lax.rem(pos + n, S)
            return remote(m["q_send"].at[peer], m["q_recv"].at[pos], m["q_ss"].at[n], m["q_rs"].at[n], seq=peer)

        def arrive(buf, rs, n):
            src = lax.rem(pos + S - n, S)
            remote(m[buf].at[src], m[buf].at[src], m[rs].at[n], m[rs].at[n], seq=src).wait_recv()

        has_up = o + 1 < L
        has_down = o > 0

        def up(t):
            return cut_copy(o - t, m["up_ss"].at[t], pos + 2)

        def down(t):
            return cut_copy(o + t, m["down_ss"].at[t], pos - 2)

        def across(outer):
            return cut_copy(outer, m["across_ss"].at[outer], o * 2 + 1 - i)

        per = -(-(S - 1) // L)
        groups = [list(range(1, S))[n * per : (n + 1) * per] for n in range(L)]

        pl.when(has_up)(lambda: up(0).start())
        pl.when(has_down)(lambda: down(0).start())
        across(o).start()
        for n in groups[0]:
            kv_copy(n).start()
        own_kv = local(m["kv_send"].at[pos], m["kv_recv"].at[pos], m["own_sem"].at[0])
        own_kv.start()

        loads[2].wait()
        for h in range(H):
            for s in range(S):
                m["q_send"][s, h] = q[q_idx[h][s], :, cols(h)]
        own_q = local(m["q_send"].at[pos], m["q_recv"].at[pos], m["own_sem"].at[1])
        own_q.start()
        loads[3].wait()
        for h in range(H):
            m["gain_t"][h] = jnp.broadcast_to(gain[:, cols(h)], (BLOCK, W)).T
            m["gain_acc"][h] = jnp.zeros((W, BLOCK), F32)

        def turn(b, carry):
            for h in range(H):
                m["g_t"][h, b] = g[b, :, cols(h)].astype(F32).T.astype(BF16)
            return carry

        lax.fori_loop(0, NB, turn, 0)

        for t in range(L - 1):
            below = o - 1 - t
            above = o + 1 + t

            @pl.when(below >= 0)
            def _(below=below, t=t):
                cut_arrive(below * 2 + i)
                pl.when(has_up)(lambda: up(t + 1).start())
                across(below).start()

            @pl.when(above < L)
            def _(above=above, t=t):
                cut_arrive(above * 2 + i)
                pl.when(has_down)(lambda: down(t + 1).start())
                across(above).start()

            for n in groups[t + 1]:
                kv_copy(n).start()
        for n in range(1, S):
            q_copy(n).start()
        for outer in range(L):
            cut_arrive(outer * 2 + 1 - i)
        for h in range(H):
            for c in range(KCUT):
                m["ck"][h, c * BLOCK : (c + 1) * BLOCK] = m["cut"][cut_dev[h][c], h, :, :W]
                m["cv"][h, c * BLOCK : (c + 1) * BLOCK] = m["cut"][cut_dev[h][c], h, :, W:]

        def part_a(b, carry):
            for h in range(H):
                query = q[b, :, cols(h)]
                s = dot(k[b, :, cols(h)], query, NT)
                m["s_buf"][h, 0] = s
                top = jnp.max(s, axis=0, keepdims=True) * factor
                for c in range(KCUT):
                    s = dot(m["ck"][h, c * BLOCK : (c + 1) * BLOCK], query, NT)
                    m["s_buf"][h, 1 + c] = s
                    top = jnp.maximum(top, jnp.max(s, axis=0, keepdims=True) * factor - closed[h][c])
                e = jnp.exp2(m["s_buf"][h, 0] * factor - top)
                total = jnp.sum(e, axis=0, keepdims=True)
                acc = dot(v[b, :, cols(h)], e.astype(BF16), TN)
                for c in range(KCUT):
                    e = jnp.exp2(m["s_buf"][h, 1 + c] * factor - (top + closed[h][c]))
                    total = total + jnp.sum(e, axis=0, keepdims=True)
                    acc = acc + dot(m["cv"][h, c * BLOCK : (c + 1) * BLOCK], e.astype(BF16), TN)
                m["acc"][h, b] = acc
                m["soft"][h, b] = jnp.concatenate([top, total, jnp.zeros((6, BLOCK), F32)], axis=0)
            return carry

        lax.fori_loop(0, NB, part_a, 0)

        own_kv.wait()
        for n in range(1, S):
            arrive("kv_recv", "kv_rs", n)

        def part_b(b, carry):
            square = jnp.zeros((1, BLOCK), F32)
            mix = jnp.zeros((1, BLOCK), F32)
            for h in range(H):
                slot = lax.div(perm[h, pos * NB + b], NB)
                query = q[b, :, cols(h)]
                s = dot(m["kv_recv"][slot, h, :, :W], query, NT)
                soft = m["soft"][h, b]
                old = soft[0:1]
                top = jnp.maximum(old, jnp.max(s, axis=0, keepdims=True) * factor)
                alpha = jnp.exp2(old - top)
                e = jnp.exp2(s * factor - top)
                total = soft[1:2] * alpha + jnp.sum(e, axis=0, keepdims=True)
                acc = m["acc"][h, b] * alpha + dot(m["kv_recv"][slot, h, :, W:], e.astype(BF16), TN)
                attn = (acc / total).astype(BF16)
                m["attn_t"][h, b] = attn
                attn = attn.astype(F32)
                lse = top + jnp.log2(total)
                m["soft"][h, b] = jnp.concatenate([lse, jnp.zeros((7, BLOCK), F32)], axis=0)
                square = square + jnp.sum(attn * attn, axis=0, keepdims=True)
                mix = mix + jnp.sum(
                    m["gain_t"][h] * m["g_t"][h, b].astype(F32) * attn, axis=0, keepdims=True
                )
            m["sum_mine"][pl.ds(b, 1), :] = square
            m["sum_mine"][pl.ds(NB + b, 1), :] = mix
            return carry

        lax.fori_loop(0, NB, part_b, 0)

        def sum_copy(n):
            return remote(
                m["sum_mine"], m["sum_recv"].at[n], m["sum_ss"].at[n], m["sum_rs"].at[n], head=lax.rem(hpos + n, HD)
            )

        for n in range(1, HD):
            sum_copy(n).start()
        sums = m["sum_mine"][...]
        for n in range(1, HD):
            sum_copy(n).wait_recv()
        for n in range(1, HD):
            sums = sums + m["sum_recv"][n]
        scale_rows = lax.rsqrt(sums[:NB] / features + 1e-06)
        m["row"][:NB] = scale_rows
        m["row"][NB:] = scale_rows * scale_rows * scale_rows * sums[NB:] / features

        def part_c(b, carry):
            scale_row = m["row"][pl.ds(b, 1), :]
            coef = m["row"][pl.ds(NB + b, 1), :]
            pieces = []
            for h in range(H):
                attn = m["attn_t"][h, b].astype(F32)
                grad = m["g_t"][h, b].astype(F32)
                gain_t = m["gain_t"][h]
                scaled = attn * scale_row
                m["norm_buf"][b, :, cols(h)] = (scaled * gain_t).T.astype(BF16)
                cot = (scale_row * gain_t * grad - attn * coef).astype(BF16).astype(F32)
                m["cot"][h, b] = cot.T.astype(BF16)
                delta = jnp.sum(cot * attn, axis=0, keepdims=True)
                m["gain_acc"][h] = m["gain_acc"][h] + grad * scaled
                pieces += [m["soft"][h, b, 0:1], delta]
            pieces.append(jnp.zeros((d.stat_rows - len(pieces), BLOCK), F32))
            m["stat"][b] = jnp.concatenate(pieces, axis=0)
            return carry

        lax.fori_loop(0, NB, part_c, 0)
        out_norm = local(m["norm_buf"], norm_hbm, m["out_sem"].at[0])
        out_norm.start()

        for s in range(S):
            for h in range(H):
                m["cot_send"][s, h] = m["cot"][h, q_idx[h][s]]
                m["cst_send"][s, 2 * h : 2 * h + 2] = m["stat"][q_idx[h][s]][2 * h : 2 * h + 2]
            m["cst_send"][s, 2 * H :] = jnp.zeros((d.stat_rows - 2 * H, BLOCK), F32)
        m["gain_mine"][...] = jnp.concatenate(
            [
                jnp.broadcast_to(jnp.sum(m["gain_acc"][h], axis=1, keepdims=True), (W, BLOCK)).T[:8]
                for h in range(H)
            ],
            axis=1,
        )

        def cot_copy(n):
            peer = lax.rem(pos + n, S)
            return remote(m["cot_send"].at[peer], m["cot_recv"].at[pos], m["cot_ss"].at[n], m["cot_rs"].at[n], seq=peer)

        def cst_copy(n):
            peer = lax.rem(pos + n, S)
            return remote(m["cst_send"].at[peer], m["cst_recv"].at[pos], m["cst_ss"].at[n], m["cst_rs"].at[n], seq=peer)

        def gain_copy(n):
            peer = lax.rem(pos + n, S)
            return remote(m["gain_mine"], m["gain_recv"].at[n], m["gain_ss"].at[n], m["gain_rs"].at[n], seq=peer)

        for n in range(1, S):
            cot_copy(n).start()
            cst_copy(n).start()
        own_cot = local(m["cot_send"].at[pos], m["cot_recv"].at[pos], m["own_sem"].at[2])
        own_cst = local(m["cst_send"].at[pos], m["cst_recv"].at[pos], m["own_sem"].at[3])
        own_cot.start()
        own_cst.start()
        for n in range(1, S):
            gain_copy(n).start()

        def terms(keys, values, query, cot, lse, delta):
            prob = jnp.exp2(dot(keys, query, NT) * factor - lse)
            dscore = (prob * (dot(values, cot, NT) - delta)).astype(BF16)
            return prob.astype(BF16), dscore

        def cut_backward(h):
            m["cut_sum"][h] = jnp.zeros((KCUT, BLOCK, 2 * W), F32)

            def step(b, carry):
                query = q[b, :, cols(h)]
                cot = m["cot"][h, b]
                stat = m["stat"][b]
                lse = stat[2 * h : 2 * h + 1]
                delta = stat[2 * h + 1 : 2 * h + 2]
                dq = jnp.zeros((W, BLOCK), F32)
                for c in range(KCUT):
                    keys = m["ck"][h, c * BLOCK : (c + 1) * BLOCK]
                    values = m["cv"][h, c * BLOCK : (c + 1) * BLOCK]
                    prob, dscore = terms(keys, values, query, cot, lse + closed[h][c], delta)
                    dq = dq + dot(keys, dscore, TN)
                    m["cut_sum"][h, c, :, :W] = m["cut_sum"][h, c, :, :W] + dot(dscore, query, NN)
                    m["cut_sum"][h, c, :, W:] = m["cut_sum"][h, c, :, W:] + dot(prob, cot, NN)
                m["acc"][h, b] = dq
                return carry

            lax.fori_loop(0, NB, step, 0)

        def term_of(h, slot):
            c = jnp.int32(0)
            for n in range(KCUT):
                c = jnp.where(cut_dev[h][n] == slot, n, c)
            return c

        def cut_part(h, slot):
            part = m["cut_sum"][h, term_of(h, slot)]
            return jnp.concatenate([part[:, :W] * scale, part[:, W:]], axis=1)

        def x_copy(h):
            return remote(m["x_send"].at[h], m["x_recv"].at[h], m["x_ss"].at[h], m["x_rs"].at[h], seq=o * 2 + 1 - i)

        def z_copy(h, n):
            peer = lax.rem(o + n, L)
            return remote(
                m["z_send"].at[h, peer], m["z_recv"].at[h, n], m["z_ss"].at[h, n], m["z_rs"].at[h, n], seq=peer * 2 + i
            )

        def x_start(h):
            for outer in range(L):
                m["x_send"][h, outer] = cut_part(h, outer * 2 + 1 - i).astype(BF16)
            x_copy(h).start()

        def z_start(h):
            x_copy(h).wait_recv()
            for outer in range(L):
                m["z_send"][h, outer] = (cut_part(h, outer * 2 + i) + m["x_recv"][h, outer].astype(F32)).astype(BF16)
            for n in range(1, L):
                z_copy(h, n).start()

        for h in range(H):
            cut_backward(h)
            x_start(h)

        def near(b, carry):
            stat = m["stat"][b]
            for h in range(H):
                query = q[b, :, cols(h)]
                cot = m["cot"][h, b]
                lse = stat[2 * h : 2 * h + 1]
                delta = stat[2 * h + 1 : 2 * h + 2]
                keys = k[b, :, cols(h)]
                prob, dscore = terms(keys, v[b, :, cols(h)], query, cot, lse, delta)
                dq = m["acc"][h, b] + dot(keys, dscore, TN)
                m["dkv"][b, h, :, :W] = dot(dscore, query, NN) * scale
                m["dkv"][b, h, :, W:] = dot(prob, cot, NN)
                slot = lax.div(perm[h, pos * NB + b], NB)
                keys = m["kv_recv"][slot, h, :, :W]
                prob, dscore = terms(keys, m["kv_recv"][slot, h, :, W:], query, cot, lse, delta)
                dq = dq + dot(keys, dscore, TN)
                m["dq_buf"][b, :, cols(h)] = (dq * scale).T.astype(BF16)
            return carry

        lax.fori_loop(0, NB, near, 0)
        out_dq = local(m["dq_buf"], dq_hbm, m["out_sem"].at[1])
        out_dq.start()
        for h in range(H):
            z_start(h)

        own_q.wait()
        own_cot.wait()
        own_cst.wait()
        for n in range(1, S):
            arrive("q_recv", "q_rs", n)
            arrive("cot_recv", "cot_rs", n)
            arrive("cst_recv", "cst_rs", n)

        def far(b, carry):
            for h in range(H):
                slot = jnp.int32(0)
                for s in range(S):
                    slot = jnp.where(slot_of[h][s] == b, s, slot)
                query = m["q_recv"][slot, h]
                cot = m["cot_recv"][slot, h]
                stat = m["cst_recv"][slot]
                lse = stat[2 * h : 2 * h + 1]
                delta = stat[2 * h + 1 : 2 * h + 2]
                prob, dscore = terms(k[b, :, cols(h)], v[b, :, cols(h)], query, cot, lse, delta)
                m["dkv"][b, h, :, :W] = m["dkv"][b, h, :, :W] + (dot(dscore, query, NN) * scale).astype(BF16).astype(F32)
                m["dkv"][b, h, :, W:] = m["dkv"][b, h, :, W:] + dot(prob, cot, NN).astype(BF16).astype(F32)
            return carry

        lax.fori_loop(0, NB, far, 0)

        gain_total = m["gain_mine"][...]
        for n in range(1, S):
            gain_copy(n).wait_recv()
        for n in range(1, S):
            gain_total = gain_total + m["gain_recv"][n]
        gain_out[...] = gain_total[:1]

        for h in range(H):
            for n in range(1, L):
                z_copy(h, n).wait_recv()
            total = m["z_send"][h, o].astype(F32)
            for n in range(1, L):
                total = total + m["z_recv"][h, n].astype(F32)
            m["cut_sum"][h, 0] = total

        def final(b, carry):
            for h in range(H):
                grad = m["dkv"][b, h]
                hit = jnp.logical_and(cut_has[h] > 0, cut_local[h] == b)
                grad = grad + jnp.where(hit, jnp.float32(1), jnp.float32(0)) * m["cut_sum"][h, 0]
                m["dk_buf"][b, :, cols(h)] = grad[:, :W].astype(BF16)
                m["dv_buf"][b, :, cols(h)] = grad[:, W:].astype(BF16)
            return carry

        lax.fori_loop(0, NB, final, 0)
        out_dk = local(m["dk_buf"], dk_hbm, m["out_sem"].at[2])
        out_dv = local(m["dv_buf"], dv_hbm, m["out_sem"].at[3])
        out_dk.start()
        out_dv.start()

        for t in range(L):

            @pl.when(jnp.logical_and(has_up, o - t >= 0))
            def _(t=t):
                up(t).wait_send()

            @pl.when(jnp.logical_and(has_down, o + t < L))
            def _(t=t):
                down(t).wait_send()

            across(t).wait_send()
        for n in range(1, S):
            kv_copy(n).wait_send()
            q_copy(n).wait_send()
            cot_copy(n).wait_send()
            cst_copy(n).wait_send()
            gain_copy(n).wait_send()
        for n in range(1, HD):
            sum_copy(n).wait_send()
        for h in range(H):
            x_copy(h).wait_send()
            for n in range(1, L):
                z_copy(h, n).wait_send()
        out_norm.wait()
        out_dq.wait()
        out_dk.wait()
        out_dv.wait()

    return kernel


def layer(query_rows, key_rows, value_rows, out_grad, block_perm, cut_count, norm_gain):
    heads = block_perm.shape[0]
    width = query_rows.shape[1] // heads
    d = Dims(
        heads, width, query_rows.shape[0] // BLOCK, lax.axis_size("seq"), lax.axis_size("head")
    )
    scratch = scratch_of(d)
    hbm = pl.BlockSpec(memory_space=pl.ANY)
    smem = pl.BlockSpec(memory_space=pltpu.SMEM)
    vmem = pl.BlockSpec(memory_space=pltpu.VMEM)
    tokens = query_rows.shape[0]
    tiled = (d.blocks, BLOCK, heads * width)
    rows = jax.ShapeDtypeStruct(tiled, BF16)
    outs = pl.pallas_call(
        make_kernel(d, list(scratch)),
        in_specs=[smem, smem, hbm, hbm, hbm, hbm, vmem],
        out_specs=[hbm, hbm, hbm, hbm, vmem],
        out_shape=[rows, rows, rows, rows, jax.ShapeDtypeStruct((1, heads * width), F32)],
        scratch_shapes=list(scratch.values()),
        compiler_params=pltpu.CompilerParams(
            collective_id=0, has_side_effects=True, vmem_limit_bytes=VMEM_LIMIT
        ),
        cost_estimate=pl.CostEstimate(
            flops=int(2 * tokens * BLOCK * heads * width * 44), bytes_accessed=int(16 * tokens * heads * width),
            transcendentals=0,
        ),
        name="layer",
    )(
        block_perm,
        cut_count,
        *[x.reshape(tiled) for x in (query_rows, key_rows, value_rows, out_grad)],
        norm_gain.reshape(1, heads * width),
    )
    return *[x.reshape(tokens, heads * width) for x in outs[:4]], outs[4].reshape(heads * width)


def solution(mesh):
    rows = P("seq", "head")
    return jax.shard_map(
        layer,
        mesh=mesh,
        in_specs=(rows, rows, rows, rows, P("head", None), P("head"), P("head")),
        out_specs=(rows, rows, rows, rows, P("head")),
        check_vma=False,
    )
```

```python
import math

import jax
import jax.numpy as jnp
from jax import lax
from jax.experimental import pallas as pl
from jax.experimental.pallas import tpu as pltpu
from jax.sharding import PartitionSpec as P

BLOCK = 256
KCUT = 4
F32 = jnp.float32
BF16 = jnp.bfloat16
NT = (((1,), (1,)), ((), ()))
TN = (((0,), (0,)), ((), ()))
NN = (((1,), (0,)), ((), ()))
VMEM_LIMIT = 60 * 1024 * 1024
MESH = pl.DeviceIdType.MESH


def dot(a, b, dims):
    return lax.dot_general(a, b, dims, preferred_element_type=F32)


class Dims:
    def __init__(self, heads, width, blocks, slots, head_devs):
        self.heads = heads
        self.width = width
        self.blocks = blocks
        self.slots = slots
        self.head_devs = head_devs
        self.inner = 2
        self.outer = slots // 2
        self.stat_rows = 8 * (-(-2 * heads // 8))


def scratch_of(d):
    H, W, NB, S, L = d.heads, d.width, d.blocks, d.slots, d.outer
    dma = pltpu.SemaphoreType.DMA
    return dict(
        q=pltpu.VMEM((NB, BLOCK, H * W), BF16),
        k=pltpu.VMEM((NB, BLOCK, H * W), BF16),
        v=pltpu.VMEM((NB, BLOCK, H * W), BF16),
        g=pltpu.VMEM((NB, BLOCK, H * W), BF16),
        kv_send=pltpu.VMEM((S, H, BLOCK, 2 * W), BF16),
        kv_recv=pltpu.VMEM((S, H, BLOCK, 2 * W), BF16),
        cut=pltpu.VMEM((S, H, BLOCK, 2 * W), BF16),
        q_send=pltpu.VMEM((S, H, BLOCK, W), BF16),
        q_recv=pltpu.VMEM((S, H, BLOCK, W), BF16),
        cot_send=pltpu.VMEM((S, H, BLOCK, W), BF16),
        cot_recv=pltpu.VMEM((S, H, BLOCK, W), BF16),
        cst_send=pltpu.VMEM((S, d.stat_rows, BLOCK), F32),
        cst_recv=pltpu.VMEM((S, d.stat_rows, BLOCK), F32),
        ck=pltpu.VMEM((H, KCUT * BLOCK, W), BF16),
        cv=pltpu.VMEM((H, KCUT * BLOCK, W), BF16),
        s_buf=pltpu.VMEM((H, 1 + KCUT, BLOCK, BLOCK), F32),
        acc=pltpu.VMEM((H, NB, W, BLOCK), F32),
        soft=pltpu.VMEM((H, NB, 8, BLOCK), F32),
        attn_t=pltpu.VMEM((H, NB, W, BLOCK), BF16),
        g_t=pltpu.VMEM((H, NB, W, BLOCK), BF16),
        gain_t=pltpu.VMEM((H, W, BLOCK), F32),
        gain_acc=pltpu.VMEM((H, W, BLOCK), F32),
        sum_mine=pltpu.VMEM((2 * NB, BLOCK), F32),
        sum_recv=pltpu.VMEM((d.head_devs, 2 * NB, BLOCK), F32),
        row=pltpu.VMEM((2 * NB, BLOCK), F32),
        stat=pltpu.VMEM((NB, d.stat_rows, BLOCK), F32),
        cot=pltpu.VMEM((H, NB, BLOCK, W), BF16),
        cut_sum=pltpu.VMEM((H, KCUT, BLOCK, 2 * W), F32),
        x_send=pltpu.VMEM((H, L, BLOCK, 2 * W), BF16),
        x_recv=pltpu.VMEM((H, L, BLOCK, 2 * W), BF16),
        z_send=pltpu.VMEM((H, L, BLOCK, 2 * W), BF16),
        z_recv=pltpu.VMEM((H, L, BLOCK, 2 * W), BF16),
        dkv=pltpu.VMEM((NB, H, BLOCK, 2 * W), F32),
        gain_mine=pltpu.VMEM((8, H * W), F32),
        gain_recv=pltpu.VMEM((S, 8, H * W), F32),
        norm_buf=pltpu.VMEM((NB, BLOCK, H * W), BF16),
        dq_buf=pltpu.VMEM((NB, BLOCK, H * W), BF16),
        dk_buf=pltpu.VMEM((NB, BLOCK, H * W), BF16),
        dv_buf=pltpu.VMEM((NB, BLOCK, H * W), BF16),
        in_sem=dma((4,)),
        out_sem=dma((4,)),
        own_sem=dma((4,)),
        kv_ss=dma((S,)),
        kv_rs=dma((S,)),
        q_ss=dma((S,)),
        q_rs=dma((S,)),
        cot_ss=dma((S,)),
        cot_rs=dma((S,)),
        cst_ss=dma((S,)),
        cst_rs=dma((S,)),
        up_ss=dma((L, H)),
        down_ss=dma((L, H)),
        across_ss=dma((L, H)),
        cut_rs=dma((S, H)),
        sum_ss=dma((d.head_devs,)),
        sum_rs=dma((d.head_devs,)),
        x_ss=dma((H,)),
        x_rs=dma((H,)),
        z_ss=dma((H, L)),
        z_rs=dma((H, L)),
        gain_ss=dma((S,)),
        gain_rs=dma((S,)),
    )


def make_kernel(d, names):
    H, W, NB, S, L, HD = d.heads, d.width, d.blocks, d.slots, d.outer, d.head_devs
    features = HD * H * W
    scale = W ** (-0.5)
    factor = scale * math.log2(math.e)

    def cols(h):
        return slice(h * W, (h + 1) * W)

    def kernel(perm, count, q_hbm, k_hbm, v_hbm, g_hbm, gain, norm_hbm, dq_hbm, dk_hbm, dv_hbm, gain_out, *scratch):
        m = dict(zip(names, scratch))
        pos = lax.axis_index("seq")
        hpos = lax.axis_index("head")
        o = lax.div(pos, 2)
        i = lax.rem(pos, 2)

        def local(src, dst, sem):
            return pltpu.make_async_copy(src, dst, sem)

        def remote(src, dst, ss, rs, seq=None, head=None):
            target = {"seq": seq} if seq is not None else {"head": head}
            return pltpu.make_async_remote_copy(
                src_ref=src, dst_ref=dst, send_sem=ss, recv_sem=rs, device_id=target, device_id_type=MESH
            )

        loads = [
            local(src, m[name], m["in_sem"].at[n])
            for n, (src, name) in enumerate([(k_hbm, "k"), (v_hbm, "v"), (q_hbm, "q"), (g_hbm, "g")])
        ]
        for copy in loads:
            copy.start()

        barrier = pltpu.get_barrier_semaphore()
        for n in range(1, S):
            pl.semaphore_signal(barrier, inc=1, device_id={"seq": lax.rem(pos + n, S)}, device_id_type=MESH)
        for n in range(1, HD):
            pl.semaphore_signal(barrier, inc=1, device_id={"head": lax.rem(hpos + n, HD)}, device_id_type=MESH)

        kv_idx = []
        q_idx = []
        slot_of = []
        for h in range(H):
            kv_row = []
            q_row = []
            slot_row = []
            for s in range(S):
                idx = jnp.int32(0)
                qi = jnp.int32(0)
                valid = jnp.int32(-1)
                for b in range(NB):
                    p = perm[h, s * NB + b]
                    mine = lax.div(p, NB) == pos
                    idx = jnp.where(mine, lax.rem(p, NB), idx)
                    valid = jnp.where(mine, lax.rem(p, NB), valid)
                    there = lax.div(perm[h, pos * NB + b], NB) == s
                    qi = jnp.where(there, b, qi)
                slot_row.append(valid)
                kv_row.append(idx)
                q_row.append(qi)
            kv_idx.append(kv_row)
            q_idx.append(q_row)
            slot_of.append(slot_row)
        cut_dev = [[lax.div(perm[h, c], NB) for c in range(KCUT)] for h in range(H)]
        cut_local = []
        cut_has = []
        closed = []
        for h in range(H):
            where = jnp.int32(0)
            has = jnp.int32(0)
            for c in range(KCUT):
                mine = cut_dev[h][c] == pos
                where = jnp.where(mine, lax.rem(perm[h, c], NB), where)
                has = jnp.where(mine, 1, has)
            cut_local.append(where)
            cut_has.append(has)
            closed.append([jnp.where(count[h] > c, jnp.float32(0), jnp.float32(1e30)) for c in range(KCUT)])

        loads[0].wait()
        loads[1].wait()
        k, v, q, g = m["k"], m["v"], m["q"], m["g"]
        for h in range(H):
            r = cut_local[h]
            m["cut"][pos, h, :, :W] = k[r, :, cols(h)]
            m["cut"][pos, h, :, W:] = v[r, :, cols(h)]
        pl.semaphore_wait(barrier, S - 1 + HD - 1)

        def cut_copy(h, outer, sem, target):
            slot = outer * 2 + i
            return remote(m["cut"].at[slot, h], m["cut"].at[slot, h], sem, m["cut_rs"].at[slot, h], seq=target)

        def cut_arrive(h, slot):
            remote(
                m["cut"].at[slot, h], m["cut"].at[slot, h], m["across_ss"].at[0, h], m["cut_rs"].at[slot, h], seq=pos
            ).wait_recv()

        steps = [L // 2] + [n for n in range(1, L) if n != L // 2]
        hops = [None] + [(n, 0) for n in steps] + [(n, 1) for n in steps] + [(0, 1)]

        def peer_of(n):
            return lax.rem(o + hops[n][0], L) * 2 + lax.rem(i + hops[n][1], 2)

        def source_of(n):
            return lax.rem(o + L - hops[n][0], L) * 2 + lax.rem(i + hops[n][1], 2)

        def kv_copy(n):
            peer = peer_of(n)
            return remote(m["kv_send"].at[peer], m["kv_recv"].at[pos], m["kv_ss"].at[n], m["kv_rs"].at[n], seq=peer)

        def q_copy(n):
            peer = peer_of(n)
            return remote(m["q_send"].at[peer], m["q_recv"].at[pos], m["q_ss"].at[n], m["q_rs"].at[n], seq=peer)

        def arrive(buf, rs, n):
            src = source_of(n)
            remote(m[buf].at[src], m[buf].at[src], m[rs].at[n], m[rs].at[n], seq=src).wait_recv()

        has_up = o + 1 < L
        has_down = o > 0

        def up(t, h):
            return cut_copy(h, o - t, m["up_ss"].at[t, h], pos + 2)

        def down(t, h):
            return cut_copy(h, o + t, m["down_ss"].at[t, h], pos - 2)

        def across(outer, h):
            return cut_copy(h, outer, m["across_ss"].at[outer, h], o * 2 + 1 - i)

        for h in range(H):
            pl.when(has_up)(lambda h=h: up(0, h).start())
            pl.when(has_down)(lambda h=h: down(0, h).start())
            across(o, h).start()
        for h in range(H):
            for s in range(S):
                r = kv_idx[h][s]
                m["kv_send"][s, h, :, :W] = k[r, :, cols(h)]
                m["kv_send"][s, h, :, W:] = v[r, :, cols(h)]
        own_kv = local(m["kv_send"].at[pos], m["kv_recv"].at[pos], m["own_sem"].at[0])
        own_kv.start()

        loads[2].wait()
        for h in range(H):
            for s in range(S):
                m["q_send"][s, h] = q[q_idx[h][s], :, cols(h)]
        own_q = local(m["q_send"].at[pos], m["q_recv"].at[pos], m["own_sem"].at[1])
        own_q.start()
        loads[3].wait()
        for h in range(H):
            m["gain_t"][h] = jnp.broadcast_to(gain[:, cols(h)], (BLOCK, W)).T
            m["gain_acc"][h] = jnp.zeros((W, BLOCK), F32)

        def turn(b, carry):
            for h in range(H):
                m["g_t"][h, b] = g[b, :, cols(h)].astype(F32).T.astype(BF16)
            return carry

        lax.fori_loop(0, NB, turn, 0)

        def send_pairs():
            for n in range(1, S):
                kv_copy(n).start()
            for n in range(1, S):
                q_copy(n).start()

        for t in range(L - 1):
            below = o - 1 - t
            above = o + 1 + t
            if t == L - 2:
                send_pairs()
            for h in range(H):

                @pl.when(below >= 0)
                def _(below=below, t=t, h=h):
                    cut_arrive(h, below * 2 + i)
                    if t < L - 2:
                        pl.when(has_up)(lambda: up(t + 1, h).start())
                    across(below, h).start()

                @pl.when(above < L)
                def _(above=above, t=t, h=h):
                    cut_arrive(h, above * 2 + i)
                    if t < L - 2:
                        pl.when(has_down)(lambda: down(t + 1, h).start())
                    across(above, h).start()

        for outer in range(L):
            for h in range(H):
                cut_arrive(h, outer * 2 + 1 - i)
        for h in range(H):
            for c in range(KCUT):
                m["ck"][h, c * BLOCK : (c + 1) * BLOCK] = m["cut"][cut_dev[h][c], h, :, :W]
                m["cv"][h, c * BLOCK : (c + 1) * BLOCK] = m["cut"][cut_dev[h][c], h, :, W:]

        def part_a(b, carry):
            for h in range(H):
                query = q[b, :, cols(h)]
                s = dot(k[b, :, cols(h)], query, NT)
                m["s_buf"][h, 0] = s
                top = jnp.max(s, axis=0, keepdims=True) * factor
                for c in range(KCUT):
                    s = dot(m["ck"][h, c * BLOCK : (c + 1) * BLOCK], query, NT)
                    m["s_buf"][h, 1 + c] = s
                    top = jnp.maximum(top, jnp.max(s, axis=0, keepdims=True) * factor - closed[h][c])
                e = jnp.exp2(m["s_buf"][h, 0] * factor - top)
                total = jnp.sum(e, axis=0, keepdims=True)
                acc = dot(v[b, :, cols(h)], e.astype(BF16), TN)
                for c in range(KCUT):
                    e = jnp.exp2(m["s_buf"][h, 1 + c] * factor - (top + closed[h][c]))
                    total = total + jnp.sum(e, axis=0, keepdims=True)
                    acc = acc + dot(m["cv"][h, c * BLOCK : (c + 1) * BLOCK], e.astype(BF16), TN)
                m["acc"][h, b] = acc
                m["soft"][h, b] = jnp.concatenate([top, total, jnp.zeros((6, BLOCK), F32)], axis=0)
            return carry

        lax.fori_loop(0, NB, part_a, 0)

        own_kv.wait()
        for n in range(1, S):
            arrive("kv_recv", "kv_rs", n)

        def part_b(b, carry):
            square = jnp.zeros((1, BLOCK), F32)
            mix = jnp.zeros((1, BLOCK), F32)
            for h in range(H):
                slot = lax.div(perm[h, pos * NB + b], NB)
                query = q[b, :, cols(h)]
                s = dot(m["kv_recv"][slot, h, :, :W], query, NT)
                soft = m["soft"][h, b]
                old = soft[0:1]
                top = jnp.maximum(old, jnp.max(s, axis=0, keepdims=True) * factor)
                alpha = jnp.exp2(old - top)
                e = jnp.exp2(s * factor - top)
                total = soft[1:2] * alpha + jnp.sum(e, axis=0, keepdims=True)
                acc = m["acc"][h, b] * alpha + dot(m["kv_recv"][slot, h, :, W:], e.astype(BF16), TN)
                attn = (acc / total).astype(BF16)
                m["attn_t"][h, b] = attn
                attn = attn.astype(F32)
                lse = top + jnp.log2(total)
                m["soft"][h, b] = jnp.concatenate([lse, jnp.zeros((7, BLOCK), F32)], axis=0)
                square = square + jnp.sum(attn * attn, axis=0, keepdims=True)
                mix = mix + jnp.sum(
                    m["gain_t"][h] * m["g_t"][h, b].astype(F32) * attn, axis=0, keepdims=True
                )
            m["sum_mine"][pl.ds(b, 1), :] = square
            m["sum_mine"][pl.ds(NB + b, 1), :] = mix
            return carry

        lax.fori_loop(0, NB, part_b, 0)

        def sum_copy(n):
            return remote(
                m["sum_mine"], m["sum_recv"].at[n], m["sum_ss"].at[n], m["sum_rs"].at[n], head=lax.rem(hpos + n, HD)
            )

        for n in range(1, HD):
            sum_copy(n).start()
        sums = m["sum_mine"][...]
        for n in range(1, HD):
            sum_copy(n).wait_recv()
        for n in range(1, HD):
            sums = sums + m["sum_recv"][n]
        scale_rows = lax.rsqrt(sums[:NB] / features + 1e-06)
        m["row"][:NB] = scale_rows
        m["row"][NB:] = scale_rows * scale_rows * scale_rows * sums[NB:] / features

        def part_c(b, carry):
            scale_row = m["row"][pl.ds(b, 1), :]
            coef = m["row"][pl.ds(NB + b, 1), :]
            pieces = []
            for h in range(H):
                attn = m["attn_t"][h, b].astype(F32)
                grad = m["g_t"][h, b].astype(F32)
                gain_t = m["gain_t"][h]
                scaled = attn * scale_row
                m["norm_buf"][b, :, cols(h)] = (scaled * gain_t).T.astype(BF16)
                cot = (scale_row * gain_t * grad - attn * coef).astype(BF16).astype(F32)
                m["cot"][h, b] = cot.T.astype(BF16)
                delta = jnp.sum(cot * attn, axis=0, keepdims=True)
                m["gain_acc"][h] = m["gain_acc"][h] + grad * scaled
                pieces += [m["soft"][h, b, 0:1], delta]
            pieces.append(jnp.zeros((d.stat_rows - len(pieces), BLOCK), F32))
            m["stat"][b] = jnp.concatenate(pieces, axis=0)
            return carry

        lax.fori_loop(0, NB, part_c, 0)
        out_norm = local(m["norm_buf"], norm_hbm, m["out_sem"].at[0])
        out_norm.start()

        for s in range(S):
            for h in range(H):
                m["cot_send"][s, h] = m["cot"][h, q_idx[h][s]]
                m["cst_send"][s, 2 * h : 2 * h + 2] = m["stat"][q_idx[h][s]][2 * h : 2 * h + 2]
            m["cst_send"][s, 2 * H :] = jnp.zeros((d.stat_rows - 2 * H, BLOCK), F32)
        m["gain_mine"][...] = jnp.concatenate(
            [
                jnp.broadcast_to(jnp.sum(m["gain_acc"][h], axis=1, keepdims=True), (W, BLOCK)).T[:8]
                for h in range(H)
            ],
            axis=1,
        )

        def cot_copy(n):
            peer = peer_of(n)
            return remote(m["cot_send"].at[peer], m["cot_recv"].at[pos], m["cot_ss"].at[n], m["cot_rs"].at[n], seq=peer)

        def cst_copy(n):
            peer = peer_of(n)
            return remote(m["cst_send"].at[peer], m["cst_recv"].at[pos], m["cst_ss"].at[n], m["cst_rs"].at[n], seq=peer)

        def gain_copy(n):
            peer = peer_of(n)
            return remote(m["gain_mine"], m["gain_recv"].at[n], m["gain_ss"].at[n], m["gain_rs"].at[n], seq=peer)

        for n in range(1, S):
            cot_copy(n).start()
            cst_copy(n).start()
        own_cot = local(m["cot_send"].at[pos], m["cot_recv"].at[pos], m["own_sem"].at[2])
        own_cst = local(m["cst_send"].at[pos], m["cst_recv"].at[pos], m["own_sem"].at[3])
        own_cot.start()
        own_cst.start()
        for n in range(1, S):
            gain_copy(n).start()

        def terms(keys, values, query, cot, lse, delta):
            prob = jnp.exp2(dot(keys, query, NT) * factor - lse)
            dscore = (prob * (dot(values, cot, NT) - delta)).astype(BF16)
            return prob.astype(BF16), dscore

        def cut_backward(h):
            m["cut_sum"][h] = jnp.zeros((KCUT, BLOCK, 2 * W), F32)

            def step(b, carry):
                query = q[b, :, cols(h)]
                cot = m["cot"][h, b]
                stat = m["stat"][b]
                lse = stat[2 * h : 2 * h + 1]
                delta = stat[2 * h + 1 : 2 * h + 2]
                dq = jnp.zeros((W, BLOCK), F32)
                for c in range(KCUT):
                    keys = m["ck"][h, c * BLOCK : (c + 1) * BLOCK]
                    values = m["cv"][h, c * BLOCK : (c + 1) * BLOCK]
                    prob, dscore = terms(keys, values, query, cot, lse + closed[h][c], delta)
                    dq = dq + dot(keys, dscore, TN)
                    m["cut_sum"][h, c, :, :W] = m["cut_sum"][h, c, :, :W] + dot(dscore, query, NN)
                    m["cut_sum"][h, c, :, W:] = m["cut_sum"][h, c, :, W:] + dot(prob, cot, NN)
                m["acc"][h, b] = dq
                return carry

            lax.fori_loop(0, NB, step, 0)

        def term_of(h, slot):
            c = jnp.int32(0)
            for n in range(KCUT):
                c = jnp.where(cut_dev[h][n] == slot, n, c)
            return c

        def cut_part(h, slot):
            part = m["cut_sum"][h, term_of(h, slot)]
            return jnp.concatenate([part[:, :W] * scale, part[:, W:]], axis=1)

        def x_copy(h):
            return remote(m["x_send"].at[h], m["x_recv"].at[h], m["x_ss"].at[h], m["x_rs"].at[h], seq=o * 2 + 1 - i)

        def z_copy(h, n):
            peer = lax.rem(o + n, L)
            return remote(
                m["z_send"].at[h, peer], m["z_recv"].at[h, n], m["z_ss"].at[h, n], m["z_rs"].at[h, n], seq=peer * 2 + i
            )

        def x_start(h):
            for outer in range(L):
                m["x_send"][h, outer] = cut_part(h, outer * 2 + 1 - i).astype(BF16)
            x_copy(h).start()

        def z_start(h):
            x_copy(h).wait_recv()
            for outer in range(L):
                m["z_send"][h, outer] = (cut_part(h, outer * 2 + i) + m["x_recv"][h, outer].astype(F32)).astype(BF16)
            for n in range(1, L):
                z_copy(h, n).start()

        for h in range(H):
            cut_backward(h)
            x_start(h)
            if h > 0:
                z_start(h - 1)

        def near(b, carry):
            stat = m["stat"][b]
            for h in range(H):
                query = q[b, :, cols(h)]
                cot = m["cot"][h, b]
                lse = stat[2 * h : 2 * h + 1]
                delta = stat[2 * h + 1 : 2 * h + 2]
                keys = k[b, :, cols(h)]
                prob, dscore = terms(keys, v[b, :, cols(h)], query, cot, lse, delta)
                dq = m["acc"][h, b] + dot(keys, dscore, TN)
                m["dkv"][b, h, :, :W] = dot(dscore, query, NN) * scale
                m["dkv"][b, h, :, W:] = dot(prob, cot, NN)
                slot = lax.div(perm[h, pos * NB + b], NB)
                keys = m["kv_recv"][slot, h, :, :W]
                prob, dscore = terms(keys, m["kv_recv"][slot, h, :, W:], query, cot, lse, delta)
                dq = dq + dot(keys, dscore, TN)
                m["dq_buf"][b, :, cols(h)] = (dq * scale).T.astype(BF16)
            return carry

        lax.fori_loop(0, NB, near, 0)
        out_dq = local(m["dq_buf"], dq_hbm, m["out_sem"].at[1])
        out_dq.start()
        z_start(H - 1)

        own_q.wait()
        own_cot.wait()
        own_cst.wait()
        for n in range(1, S):
            arrive("q_recv", "q_rs", n)
            arrive("cot_recv", "cot_rs", n)
            arrive("cst_recv", "cst_rs", n)

        def far(b, carry):
            for h in range(H):
                slot = jnp.int32(0)
                for s in range(S):
                    slot = jnp.where(slot_of[h][s] == b, s, slot)
                query = m["q_recv"][slot, h]
                cot = m["cot_recv"][slot, h]
                stat = m["cst_recv"][slot]
                lse = stat[2 * h : 2 * h + 1]
                delta = stat[2 * h + 1 : 2 * h + 2]
                prob, dscore = terms(k[b, :, cols(h)], v[b, :, cols(h)], query, cot, lse, delta)
                m["dkv"][b, h, :, :W] = m["dkv"][b, h, :, :W] + (dot(dscore, query, NN) * scale).astype(BF16).astype(F32)
                m["dkv"][b, h, :, W:] = m["dkv"][b, h, :, W:] + dot(prob, cot, NN).astype(BF16).astype(F32)
            return carry

        lax.fori_loop(0, NB, far, 0)

        gain_total = m["gain_mine"][...]
        for n in range(1, S):
            gain_copy(n).wait_recv()
        for n in range(1, S):
            gain_total = gain_total + m["gain_recv"][n]
        gain_out[...] = gain_total[:1]

        for h in range(H):
            for n in range(1, L):
                z_copy(h, n).wait_recv()
            total = m["z_send"][h, o].astype(F32)
            for n in range(1, L):
                total = total + m["z_recv"][h, n].astype(F32)
            m["cut_sum"][h, 0] = total

        def final(b, carry):
            for h in range(H):
                grad = m["dkv"][b, h]
                hit = jnp.logical_and(cut_has[h] > 0, cut_local[h] == b)
                grad = grad + jnp.where(hit, jnp.float32(1), jnp.float32(0)) * m["cut_sum"][h, 0]
                m["dk_buf"][b, :, cols(h)] = grad[:, :W].astype(BF16)
                m["dv_buf"][b, :, cols(h)] = grad[:, W:].astype(BF16)
            return carry

        lax.fori_loop(0, NB, final, 0)
        out_dk = local(m["dk_buf"], dk_hbm, m["out_sem"].at[2])
        out_dv = local(m["dv_buf"], dv_hbm, m["out_sem"].at[3])
        out_dk.start()
        out_dv.start()

        for h in range(H):
            for t in range(L - 1):

                @pl.when(jnp.logical_and(has_up, o - t >= 0))
                def _(t=t, h=h):
                    up(t, h).wait_send()

                @pl.when(jnp.logical_and(has_down, o + t < L))
                def _(t=t, h=h):
                    down(t, h).wait_send()

            for outer in range(L):
                across(outer, h).wait_send()
        for n in range(1, S):
            kv_copy(n).wait_send()
            q_copy(n).wait_send()
            cot_copy(n).wait_send()
            cst_copy(n).wait_send()
            gain_copy(n).wait_send()
        for n in range(1, HD):
            sum_copy(n).wait_send()
        for h in range(H):
            x_copy(h).wait_send()
            for n in range(1, L):
                z_copy(h, n).wait_send()
        out_norm.wait()
        out_dq.wait()
        out_dk.wait()
        out_dv.wait()

    return kernel


def copy_kernel(*refs):
    half = len(refs) // 2
    for src, dst in zip(refs[:half], refs[half:]):
        dst[...] = src[...]


def copies(arrays):
    blocks, rows, width = arrays[0].shape
    spec = pl.BlockSpec((blocks // 2, rows, width), lambda n: (n, 0, 0))
    return pl.pallas_call(
        copy_kernel,
        grid=(2,),
        in_specs=[spec] * len(arrays),
        out_specs=[spec] * len(arrays),
        out_shape=[jax.ShapeDtypeStruct(x.shape, x.dtype) for x in arrays],
        compiler_params=pltpu.CompilerParams(vmem_limit_bytes=VMEM_LIMIT),
        name="results",
    )(*arrays)


def layer(query_rows, key_rows, value_rows, out_grad, block_perm, cut_count, norm_gain):
    heads = block_perm.shape[0]
    width = query_rows.shape[1] // heads
    d = Dims(
        heads, width, query_rows.shape[0] // BLOCK, lax.axis_size("seq"), lax.axis_size("head")
    )
    scratch = scratch_of(d)
    hbm = pl.BlockSpec(memory_space=pl.ANY)
    smem = pl.BlockSpec(memory_space=pltpu.SMEM)
    vmem = pl.BlockSpec(memory_space=pltpu.VMEM)
    tokens = query_rows.shape[0]
    tiled = (d.blocks, BLOCK, heads * width)
    rows = jax.ShapeDtypeStruct(tiled, BF16)
    outs = pl.pallas_call(
        make_kernel(d, list(scratch)),
        in_specs=[smem, smem, hbm, hbm, hbm, hbm, vmem],
        out_specs=[hbm, hbm, hbm, hbm, vmem],
        out_shape=[rows, rows, rows, rows, jax.ShapeDtypeStruct((1, heads * width), F32)],
        scratch_shapes=list(scratch.values()),
        compiler_params=pltpu.CompilerParams(
            collective_id=0, has_side_effects=True, vmem_limit_bytes=VMEM_LIMIT
        ),
        cost_estimate=pl.CostEstimate(
            flops=int(2 * tokens * BLOCK * heads * width * 44), bytes_accessed=int(16 * tokens * heads * width),
            transcendentals=0,
        ),
        name="layer",
    )(
        block_perm,
        cut_count,
        *[x.reshape(tiled) for x in (query_rows, key_rows, value_rows, out_grad)],
        norm_gain.reshape(1, heads * width),
    )
    return *[x.reshape(tokens, heads * width) for x in copies(outs[:4])], outs[4].reshape(heads * width)


def solution(mesh):
    rows = P("seq", "head")
    return jax.shard_map(
        layer,
        mesh=mesh,
        in_specs=(rows, rows, rows, rows, P("head", None), P("head"), P("head")),
        out_specs=(rows, rows, rows, rows, P("head")),
        check_vma=False,
    )
```
